256 devices in a mesh: section: 2 (over y_lo), lat: 4 (over y_hi, core), lon: 32 (over z, x).
Axes of the slice: x: 4, y: 4 (y_hi: 2, y_lo: 2; y = y_hi * 2 + y_lo), z: 8, core: 2. Of those that a mesh axis runs over, the one named last changes fastest.
Arguments:
- start: bfloat16 [2, 12, 32, 8192], P('section', None, 'lat', 'lon'), may hold values from -6 to 6
- prior_mean: bfloat16 [12, 32, 8192], P(None, 'lat', 'lon'), may hold values from -6 to 6
- lift_w: bfloat16 [2, 24, 128], P('section'), may hold values from -1.25 to 1.25
- noise_gain: float32 [2, 128], P('section'), may hold values from -8 to 8
- conv0a: bfloat16 [2, 9, 128, 128], P('section'), may hold values from -0.25 to 0.25
- expand: bfloat16 [2, 128, 256], P('section'), may hold values from -0.5 to 0.5
- conv1a: bfloat16 [2, 9, 256, 256], P('section'), may hold values from -0.1875 to 0.1875
- conv1b: bfloat16 [2, 9, 256, 256], P('section'), may hold values from -0.1875 to 0.1875
- shrink: bfloat16 [2, 256, 128], P('section'), may hold values from -0.375 to 0.375
- conv0b: bfloat16 [2, 9, 128, 128], P('section'), may hold values from -0.25 to 0.25
- head: bfloat16 [2, 128, 12], P('section'), may hold values from -0.5 to 0.5
Outputs:
- results: bfloat16 [2, 12, 32, 8192], P('section', None, 'lat', 'lon')
The draws below stay inside these ranges and needn't reach their ends.
All inputs are finite; a program needn't handle non-finite values.
Results may differ from the reference program's by a relative error of at most 0.013.
Values may be sent and summed in bfloat16 or wider, within the bound.
No kernel may reach another device: no remote copies, remote signals or barrier semaphores. Data moves between devices by JAX's collectives and lax.ppermute only.
A program may use at most 64 MiB of HBM per device.

```python
import math
import jax
import jax.numpy as jnp
from jax import lax

VARS = 12
C0 = 128
C1 = 256
HEIGHT = 32
WIDTH = 8192


def level_of(stream_key, shape, split, low, top_value):
    loudness = 1.0
    for position, parts in split:
        heights = jax.random.uniform(jax.random.fold_in(jax.random.fold_in(stream_key, 6), position), (parts,), jnp.float32, low / len(split), top_value / len(split))
        loudness = loudness * jnp.repeat(jnp.exp(heights), shape[position] // parts).reshape((-1,) + (1,) * (len(shape) - 1 - position))
    return loudness


def noise(key, shape, deviation, reach, split=(), dtype=jnp.bfloat16):
    array = jax.random.normal(key, shape, jnp.float32) * deviation
    if len(split) > 0:
        array = level_of(key, shape, split, -0.22, 0.18) * array
    return jnp.clip(array, min=-reach, max=reach).astype(dtype)


def setup_inputs(seed: int = 0) -> dict:
    splits = jax.random.split(jax.random.key(seed), 12)
    return {
        "start": noise(splits[0], (2, VARS, HEIGHT, WIDTH), 1.0, 6.0, ((0, 2), (2, 4), (3, 32))),
        "prior_mean": noise(splits[1], (VARS, HEIGHT, WIDTH), 1.0, 6.0, ((1, 4), (2, 32))),
        "lift_w": noise(splits[2], (2, 2 * VARS, C0), (2 * VARS) ** -0.5, 1.25, ((0, 2),)),
        "noise_gain": noise(splits[3], (2, C0), 2.0, 8.0, ((0, 2),), jnp.float32),
        "conv0a": noise(splits[4], (2, 9, C0, C0), (4 * C0) ** -0.5, 0.25, ((0, 2),)),
        "expand": noise(splits[5], (2, C0, C1), C0 ** -0.5, 0.5, ((0, 2),)),
        "conv1a": noise(splits[6], (2, 9, C1, C1), (4 * C1) ** -0.5, 0.1875, ((0, 2),)),
        "conv1b": noise(splits[7], (2, 9, C1, C1), (4 * C1) ** -0.5, 0.1875, ((0, 2),)),
        "shrink": noise(splits[8], (2, C1, C0), C1 ** -0.5, 0.375, ((0, 2),)),
        "conv0b": noise(splits[9], (2, 9, C0, C0), (4 * C0) ** -0.5, 0.25, ((0, 2),)),
        "head": noise(splits[10], (2, C0, VARS), C0 ** -0.5, 0.5, ((0, 2),)),
    }


sigma_data = 0.5
sigma_high = 2.0
sigma_low = 0.5

def precondition(sigma):
    total = sigma * sigma + sigma_data * sigma_data
    return (1.0 / math.sqrt(total), sigma_data * sigma_data / total, sigma * sigma_data / math.sqrt(total), math.log(sigma) / 4.0)

def pad_grid(field):
    wrapped = jnp.concatenate([field[:, -1:], field, field[:, :1]], axis=1)
    return jnp.pad(wrapped, ((1, 1), (0, 0), (0, 0)))

def convolve(padded, kernel, height, breadth):
    channels = padded.shape[-1]
    total = jnp.zeros((height * breadth, kernel.shape[-1]), jnp.float32)
    for offset in range(9):
        down, across = divmod(offset, 3)
        window = padded[down:down + height, across:across + breadth].reshape(height * breadth, channels)
        total = total + jnp.dot(window, kernel[offset], preferred_element_type=jnp.float32)
    return total.reshape(height, breadth, -1)

def network(state, prior, shift, weights):
    lift_w, conv0a, expand, conv1a, conv1b, shrink, conv0b, head = weights
    fields = jnp.concatenate([state, prior], axis=0)
    channels, height, breadth = fields.shape
    flat = fields.reshape(channels, height * breadth)
    hidden = lax.dot_general(flat, lift_w, (((0,), (0,)), ((), ())), preferred_element_type=jnp.float32)
    lifted = jax.nn.silu(hidden + shift).astype(jnp.bfloat16).reshape(height, breadth, -1)
    first_level = jax.nn.silu(convolve(pad_grid(lifted), conv0a, height, breadth)).astype(jnp.bfloat16)
    half_h = height // 2
    half_b = breadth // 2
    pooled = (lax.optimization_barrier(jnp.sum(first_level.reshape(half_h, 2, half_b, 2, -1).astype(jnp.float32), axis=(1, 3))) * 0.25).astype(jnp.bfloat16)
    widened = jnp.dot(pooled.reshape(half_h * half_b, -1), expand, preferred_element_type=jnp.float32).astype(jnp.bfloat16).reshape(half_h, half_b, -1)
    inner = jax.nn.silu(convolve(pad_grid(widened), conv1a, half_h, half_b)).astype(jnp.bfloat16)
    coarse_out = (jax.nn.silu(convolve(pad_grid(inner), conv1b, half_h, half_b)) + widened.astype(jnp.float32)).astype(jnp.bfloat16)
    projected = jnp.dot(coarse_out.reshape(half_h * half_b, -1), shrink, preferred_element_type=jnp.float32).reshape(half_h, 1, half_b, 1, -1)
    spread = jnp.broadcast_to(projected, (half_h, 2, half_b, 2, projected.shape[-1])).reshape(height, breadth, -1)
    merged = (spread + first_level.astype(jnp.float32)).astype(jnp.bfloat16)
    last_level = jax.nn.silu(convolve(pad_grid(merged), conv0b, height, breadth)).astype(jnp.bfloat16)
    output = lax.dot_general(head, last_level.reshape(height * breadth, -1), (((0,), (1,)), ((), ())), preferred_element_type=jnp.float32)
    return output.reshape(-1, height, breadth)

def reference(start, prior_mean, lift_w, noise_gain, conv0a, expand, conv1a, conv1b, shrink, conv0b, head):

    def weights_of(section):
        return (lift_w[section], conv0a[section], expand[section], conv1a[section], conv1b[section], shrink[section], conv0b[section], head[section])
    high = precondition(sigma_high)
    low = precondition(sigma_low)
    zero_shift = jnp.zeros((lift_w.shape[-1],), jnp.float32)
    mean_next = network(start[0], prior_mean, zero_shift, weights_of(0)).astype(jnp.bfloat16)
    noisy = sigma_high * start[1].astype(jnp.float32)
    first_input = (high[0] * noisy).astype(jnp.bfloat16)
    first_out = network(first_input, prior_mean, high[3] * noise_gain[1], weights_of(1))
    first_denoised = high[1] * noisy + high[2] * first_out
    moved = noisy + (sigma_low - sigma_high) / sigma_high * (noisy - first_denoised)
    second_input = (low[0] * moved).astype(jnp.bfloat16)
    second_out = network(second_input, prior_mean, low[3] * noise_gain[1], weights_of(1))
    second_denoised = low[1] * moved + low[2] * second_out
    sample = (prior_mean.astype(jnp.float32) + second_denoised).astype(jnp.bfloat16)
    return jnp.stack([sample, mean_next])
```

```python
import math

import jax
import jax.numpy as jnp
from jax import lax
from jax.experimental import pallas as pl
from jax.experimental.pallas import tpu as pltpu
from jax.sharding import PartitionSpec as P

sigma_data = 0.5
sigma_high = 2.0
sigma_low = 0.5

VARS = 12
C0 = 128
C1 = 256
F32 = jnp.float32
BF16 = jnp.bfloat16

TILE = 64
REACH = 32
KEPT = 16
COLS = TILE + 2 * KEPT
HALO1 = 13
HALO2 = 7


def precondition(sigma):
    total = sigma * sigma + sigma_data * sigma_data
    return (
        1.0 / math.sqrt(total),
        sigma_data * sigma_data / total,
        sigma * sigma_data / math.sqrt(total),
        math.log(sigma) / 4.0,
    )


def block_of(lat, lon):
    return jnp.where(lon % 2 == 0, lat, 3 - lat)


def silu(x):
    half = 0.5 * x
    return half + half * jnp.tanh(half)


def split_rows(x):
    n = x.shape[0] // 16
    y = x.reshape(n, 2, 8, x.shape[-1])
    return y[:, 0], y[:, 1]


def join_rows(low, high):
    n, _, c = low.shape
    return jnp.stack([low, high], axis=1).reshape(n * 16, c)


def from_above(x):
    low, high = split_rows(x)
    place = lax.broadcasted_iota(jnp.int32, low.shape, 1)
    low, high = pltpu.roll(low, 1, 1), pltpu.roll(high, 1, 1)
    return join_rows(jnp.where(place == 0, 0.0, low), jnp.where(place == 0, low, high))


def from_below(x):
    low, high = split_rows(x)
    place = lax.broadcasted_iota(jnp.int32, low.shape, 1)
    low, high = pltpu.roll(low, 7, 1), pltpu.roll(high, 7, 1)
    return join_rows(jnp.where(place == 7, high, low), jnp.where(place == 7, 0.0, high))


def blocks(count, size):
    return [(at, min(size, count - at)) for at in range(0, count, size)]


def pack_kernel(start, prior, own, one, two, three, start_in, prior_in, windows, sems):
    copies = [
        pltpu.make_async_copy(start.at[0], start_in, sems.at[0]),
        pltpu.make_async_copy(prior, prior_in, sems.at[1]),
    ]
    for copy in copies:
        copy.start()
    lat = lax.axis_index("lat")
    lon = lax.axis_index("lon")
    for copy in copies:
        copy.wait()
    x = jnp.concatenate([start_in[...], prior_in[...]], axis=0).astype(F32)
    left = x[:, :, :128].reshape(192, 128)
    right = x[:, :, 128:].reshape(192, 128)
    lane = lax.broadcasted_iota(jnp.int32, (192, 128), 1)
    left32, left96 = pltpu.roll(left, 32, 1), pltpu.roll(left, 96, 1)
    right32, right96 = pltpu.roll(right, 32, 1), pltpu.roll(right, 96, 1)
    windows[0] = left32
    windows[1] = jnp.where(lane < 96, left96, right96)
    windows[2] = jnp.where(lane < 32, left32, right32)
    windows[3] = right96
    for step, out in enumerate((own, one, two, three)):
        out[...] = windows[block_of(lat ^ step, lon)].reshape(24, 8, 128).astype(BF16)


def gather_kernel(own, one, two, three, state, edge, fields, cells):
    lat = lax.axis_index("lat")
    lon = lax.axis_index("lon")
    for step, piece in enumerate((own, one, two, three)):
        fields[lat ^ step] = piece[...].astype(F32).reshape(192, 128)
    pad = jnp.zeros((80, 128), F32)
    for row in range(16):
        source, first = row // 4, 2 * (row % 4)
        even = fields[source, pl.ds(first, 24, stride=8), :]
        odd = fields[source, pl.ds(first + 1, 24, stride=8), :]
        turned = jnp.concatenate([even, odd, pad], axis=0).T
        cells[pl.ds(row, COLS, stride=16), :] = turned[REACH - KEPT : REACH + TILE + KEPT]
    state[...] = cells[...].astype(BF16)
    last = block_of(lat, lon) == 3
    edge[...] = jnp.where(
        last, cells[TILE * 16 : (TILE + KEPT) * 16, :], cells[KEPT * 16 : 2 * KEPT * 16, :]
    ).astype(BF16)


def lanes_of(shape):
    lane = lax.broadcasted_iota(jnp.int32, shape, 1)
    within = jnp.where(lane < 24, lane, lane - 24)
    return within < VARS, (within >= VARS) & (lane < 48)


def load_kernel(
    after, lift_w, conv0a, expand, conv1a, conv1b, shrink, conv0b, head,
    lift2, conv0a2, expand2, conv1a2, conv1b2, shrink2, conv0b2, head2,
    small_l, small_e, small_s, small_h, sems,
):
    copies = []

    def fetch(source, target, group):
        copy = pltpu.make_async_copy(source, target, sems.at[group])
        copy.start()
        copies.append(copy)

    fetch(lift_w.at[0], small_l, 0)
    fetch(expand.at[0], small_e, 1)
    fetch(shrink.at[0], small_s, 2)
    fetch(head.at[0], small_h, 3)
    fetch(conv1a.at[0], conv1a2, 4)
    fetch(conv1b.at[0], conv1b2, 5)
    group = 6
    for weight, pairs in ((conv0a, conv0a2), (conv0b, conv0b2)):
        for across in range(3):
            for plane in range(4):
                rows = pl.ds((across * 4 + plane) * C0, C0)
                if plane < 3:
                    fetch(weight.at[0, 3 * plane + across], pairs.at[rows, pl.ds(0, C0)], group)
                    group += 1
                else:
                    pairs[rows, :C0] = jnp.zeros((C0, C0), BF16)
                if plane > 0:
                    fetch(weight.at[0, 3 * (plane - 1) + across], pairs.at[rows, pl.ds(C0, C0)], group)
                    group += 1
                else:
                    pairs[rows, C0:] = jnp.zeros((C0, C0), BF16)
    for copy in copies[:4]:
        copy.wait()
    wl = small_l[...].astype(F32)
    rest = jnp.zeros((208, C0), F32)
    none = jnp.zeros((24, C0), F32)
    lift2[...] = jnp.concatenate(
        [jnp.concatenate([wl, none, rest], axis=0), jnp.concatenate([none, wl, rest], axis=0)], axis=1
    ).astype(BF16)
    quarter = (small_e[...].astype(F32) * 0.25).astype(BF16)
    expand2[:C0, :] = quarter
    expand2[C0:, :] = quarter
    shrink2[:, :C0] = small_s[...]
    shrink2[:, C0:] = small_s[...]
    wh = small_h[...].astype(F32)
    turned = jnp.concatenate([wh, jnp.zeros((C0 - VARS, C0), F32)], axis=0).T
    empty = jnp.zeros((C0, C0), F32)
    head2[...] = jnp.concatenate(
        [
            jnp.concatenate([turned, empty], axis=1),
            jnp.concatenate([pltpu.roll(turned, 24, 1), empty], axis=1),
        ],
        axis=0,
    ).astype(BF16)
    for copy in copies[4:]:
        copy.wait()


def lanes_of(shape):
    lane = lax.broadcasted_iota(jnp.int32, shape, 1)
    within = jnp.where(lane < 24, lane, lane - 24)
    return within < VARS, (within >= VARS) & (lane < 48)


PIECE = 32
SLOTS = 32


def network_kernel(
    state, edge, gain, lift2, conv0a2, expand2, conv1a2, conv1b2, shrink2, conv0b2, head2,
    out0, out1, out2, out3,
    cells, fed, lifted, first, pooled, widened, inner, joined, merged, last, guess1, result, rows,
):
    pl.run_scoped(
        lambda *slots: network_body(
            (slots[:SLOTS], slots[SLOTS:]),
            state, edge, gain, lift2, conv0a2, expand2, conv1a2, conv1b2, shrink2, conv0b2, head2,
            (out0, out1, out2, out3),
            cells, fed, lifted, first, pooled, widened, inner, joined, merged, last, guess1, result, rows,
        ),
        *[pltpu.ACC(q)((PIECE, 256), F32) for q in (0, 1) for _ in range(SLOTS)],
    )


def network_body(
    slots, state, edge, gain, lift2, conv0a2, expand2, conv1a2, conv1b2, shrink2, conv0b2, head2,
    outs, cells, fed, lifted, first, pooled, widened, inner, joined, merged, last, guess1, result, rows,
):
    diffuse = lax.axis_index("section") == 1
    lat = lax.axis_index("lat")
    lon = lax.axis_index("lon")
    block = block_of(lat, lon)
    high = precondition(sigma_high)
    low = precondition(sigma_low)
    taken = [0, 0]
    staged = [0, 0]

    def take(q):
        slot = slots[q][taken[q] % SLOTS]
        taken[q] += 1
        return slot

    def push(q, rhs):
        pltpu.matmul_push_rhs(rhs, staging_register=staged[q], mxu_index=q)
        register = staged[q]
        staged[q] = 1 - register
        return register

    def split_rows_product(count, depth, lhs, rhs):
        held = [take(i % 2) for i in range(count)]
        for k in range(depth):
            units = range(min(2, count))
            fresh = [push(q, rhs(k)) for q in units]
            for i in range(count):
                q = i % 2
                pltpu.matmul_acc_lhs(held[i], lhs(k, i), load_staged_rhs=fresh[q])
                fresh[q] = None
        return [lambda h=h: pltpu.matmul_pop(h) for h in held]

    def split_depth_product(count, depth, lhs, rhs, first_unit):
        held = [(take(0), take(1)) for _ in range(count)]
        most = (depth + 1) // 2
        parts = [range(0, most), range(most, depth)]
        if first_unit == 1:
            parts = [range(depth - most), range(depth - most, depth)]
        for step in range(most):
            fresh = [push(q, rhs(parts[q][step])) if step < len(parts[q]) else None for q in (0, 1)]
            for i in range(count):
                for q in (0, 1):
                    if step < len(parts[q]):
                        pltpu.matmul_acc_lhs(held[i][q], lhs(parts[q][step], i), load_staged_rhs=fresh[q])
                        fresh[q] = None
        return [lambda h=h: pltpu.matmul_pop(h[0]) + pltpu.matmul_pop(h[1]) for h in held]

    left = slice(0, KEPT * 16)
    right = slice((COLS - KEPT) * 16, COLS * 16)
    middle = slice(KEPT * 16, (COLS - KEPT) * 16)
    cells[left] = jnp.where(block == 0, edge[...].astype(F32), state[left, :].astype(F32))
    cells[middle] = state[middle, :].astype(F32)
    cells[right] = jnp.where(block == 3, edge[...].astype(F32), state[right, :].astype(F32))

    is_state, is_prior = lanes_of((1, 128))
    gains = gain[...]
    enter = jnp.where(is_state, jnp.where(diffuse, sigma_high * high[0], 1.0), 1.0)
    step = (sigma_low - sigma_high) / sigma_high
    from_noise = sigma_high * (1.0 + step - step * high[1])
    from_guess = -step * high[2]
    keep = jnp.where(is_state, low[0] * from_noise, 1.0)
    add = jnp.where(is_state, low[0] * from_guess, 0.0)
    blank = jnp.zeros((PIECE, 128), BF16)

    def planes(ref, at, even, odd):
        r = slice(at * 16, at * 16 + even.shape[0])
        ref[r, 0:128] = from_above(odd).astype(BF16)
        ref[r, 128:256] = even.astype(BF16)
        ref[r, 256:384] = odd.astype(BF16)
        ref[r, 384:512] = from_below(even).astype(BF16)

    def coarse_planes(ref, at, x):
        r = slice(at * 16, at * 16 + x.shape[0])
        ref[r, 0:256] = from_above(x).astype(BF16)
        ref[r, 256:512] = x.astype(BF16)
        ref[r, 512:768] = from_below(x).astype(BF16)

    def fine(ref, at, skip=0):
        return lambda k, i: ref[
            (at + 2 * i + k // 2 + skip) * 16 : (at + 2 * i + k // 2 + skip) * 16 + PIECE,
            (k % 2) * 256 : (k % 2) * 256 + 256,
        ]

    def coarse(ref, at):
        return lambda k, i: ref[
            (at + 2 * i + k // 3) * 16 : (at + 2 * i + k // 3) * 16 + PIECE, (k % 3) * 256 : (k % 3) * 256 + 256
        ]

    def flat(ref, at):
        return lambda k, i: ref[(at + 2 * i) * 16 : (at + 2 * i) * 16 + PIECE, :]

    def tile(ref):
        return lambda k: ref[k * 256 : (k + 1) * 256, :]

    def tap(ref):
        return lambda k: ref[3 * (k % 3) + k // 3]

    def lift(at, end, prepare, shift):
        for i in range((end - at) // 2):
            fed[(at + 2 * i) * 16 : (at + 2 * i) * 16 + PIECE, :] = prepare(at + 2 * i)
        lhs = lambda k, i: jnp.concatenate([flat(fed, at)(k, i), blank], axis=1)
        pops = split_rows_product((end - at) // 2, 1, lhs, tile(lift2))
        for i, pop in enumerate(pops):
            x = silu(pop() + shift)
            planes(lifted, at + 2 * i, x[:, :C0], x[:, C0:])

    def conv_first(at, end):
        pops = split_rows_product((end - at) // 2, 6, fine(lifted, at), tile(conv0a2))
        for i, pop in enumerate(pops):
            x = silu(pop())
            c = at + 2 * i
            first[c * 16 : c * 16 + PIECE, :] = x.astype(BF16)
            pooled[c * 8 : c * 8 + 16, :] = (x[:16] + x[16:]).astype(BF16)

    def widen(at, end):
        pops = split_rows_product((end - at) // 2, 1, flat(pooled, at), tile(expand2))
        for i, pop in enumerate(pops):
            coarse_planes(widened, at + 2 * i, pop())

    def conv_inner(at, end, unit):
        pops = split_depth_product((end - at) // 2, 9, coarse(widened, at), tap(conv1a2), unit)
        for i, pop in enumerate(pops):
            coarse_planes(inner, at + 2 * i, silu(pop()))

    def conv_outer(at, end, unit):
        pops = split_depth_product((end - at) // 2, 9, coarse(inner, at), tap(conv1b2), unit)
        for i, pop in enumerate(pops):
            c = at + 2 * i
            x = silu(pop()) + widened[(c + 2) * 16 : (c + 2) * 16 + PIECE, 256:512].astype(F32)
            joined[c * 16 : c * 16 + PIECE, :] = x.astype(BF16)

    def narrow(at, end):
        pops = split_rows_product((end - at) // 2, 1, flat(joined, at), tile(shrink2))
        for i, pop in enumerate(pops):
            x = pop()
            for part in range(2):
                c = 2 * (at + 2 * i + part)
                y = x[part * 16 : part * 16 + 16]
                z = jnp.concatenate([y, y], axis=0) + first[(c + 4) * 16 : (c + 4) * 16 + PIECE, :].astype(F32)
                planes(merged, c, z[:, :C0], z[:, C0:])

    def conv_last(at, end, skip):
        pops = split_rows_product((end - at) // 2, 6, fine(merged, at, skip), tile(conv0b2))
        for i, pop in enumerate(pops):
            c = at + 2 * i
            last[c * 16 : c * 16 + PIECE, :] = silu(pop()).astype(BF16)

    def project(at, end, finish):
        pops = split_rows_product((end - at) // 2, 1, flat(last, at), tile(head2))
        for i, pop in enumerate(pops):
            finish(at + 2 * i, pop()[:, :128])

    def cut(*ends):
        return list(zip((0,) + ends, ends))

    def unet(halo, ends, shift, prepare, finish, skip):
        shift = jnp.concatenate([shift, shift], axis=1)
        n = TILE + 2 * halo
        L = cut(*[e + 2 for e in ends], n)
        A = cut(*ends, n - 2)
        E = cut(*[e // 2 for e in ends], n // 2 - 1)
        I = cut(*[e // 2 - 2 for e in ends], n // 2 - 3)
        O = cut(*[e // 2 - 4 for e in ends], n // 2 - 5)
        C = cut(*[e - 10 - 2 * skip for e in ends], n - 12 - 2 * skip)
        lift(*L[0], prepare, shift)
        yield
        lift(*L[1], prepare, shift)
        conv_first(*A[0])
        lift(*L[2], prepare, shift)
        conv_first(*A[1])
        widen(*E[0])
        conv_first(*A[2])
        widen(*E[1])
        conv_inner(*I[0], 0)
        widen(*E[2])
        conv_inner(*I[1], 1)
        conv_outer(*O[0], 0)
        conv_inner(*I[2], 0)
        conv_outer(*O[1], 1)
        narrow(*O[0])
        conv_outer(*O[2], 0)
        narrow(*O[1])
        conv_last(*C[0], skip)
        narrow(*O[2])
        conv_last(*C[1], skip)
        project(*C[0], finish)
        conv_last(*C[2], skip)
        project(*C[1], finish)
        yield
        project(*C[2], finish)

    def prepare1(c):
        at = (KEPT - HALO1 + c) * 16
        return (cells[at : at + PIECE, :] * enter).astype(BF16)

    def finish1(c, x):
        guess1[c * 16 : c * 16 + PIECE, :] = x

    def prepare2(c):
        at = (KEPT - HALO2 + c) * 16
        return (cells[at : at + PIECE, :] * keep + guess1[c * 16 : c * 16 + PIECE, :] * add).astype(BF16)

    def finish2(c, x):
        source = cells[(KEPT + c) * 16 : (KEPT + c) * 16 + PIECE, :]
        guessed = guess1[(HALO2 + c) * 16 : (HALO2 + c) * 16 + PIECE, :]
        sample = (low[1] * from_noise) * source + (low[1] * from_guess) * guessed + low[2] * x
        sample = sample + pltpu.roll(source, 128 - VARS, 1)
        result[c * 16 : c * 16 + PIECE, :] = jnp.where(diffuse, sample, guessed)

    one = unet(HALO1, (32, 60), jnp.where(diffuse, high[3], 0.0) * gains, prepare1, finish1, 0)
    two = unet(HALO2, (28, 52), low[3] * gains, prepare2, finish2, 1)
    next(one)
    next(one)
    next(two)
    for _ in one:
        pass
    for _ in two:
        pass

    for row in range(16):
        target, at = row // 4, 2 * (row % 4)
        turned = result[pl.ds(row, TILE, stride=16), :].T
        rows[target, pl.ds(at, VARS, stride=8), :] = turned[:VARS]
        rows[target, pl.ds(at + 1, VARS, stride=8), :] = turned[24 : 24 + VARS]
    for k, out in enumerate(outs):
        out[...] = rows[lat ^ k].reshape(VARS, 8, TILE).astype(BF16)


def place_kernel(in0, in1, in2, in3, out):
    lat = lax.axis_index("lat")
    lon = lax.axis_index("lon")
    pieces = [p[...].astype(F32) for p in (in0, in1, in2, in3)]
    spots = [block_of(lat ^ k, lon) for k in range(4)]
    placed = []
    for block in range(4):
        x = pieces[0]
        for k in range(1, 4):
            x = jnp.where(spots[k] == block, pieces[k], x)
        placed.append(x)
    out[0] = jnp.concatenate(placed, axis=2).astype(BF16)


def pinned(x):
    return pltpu.with_memory_space_constraint(x, pltpu.HBM)


def on_device(
    start, prior_mean, lift_w, noise_gain, conv0a, expand, conv1a, conv1b, shrink, conv0b, head
):
    lats, lons = lax.axis_size("lat"), lax.axis_size("lon")
    window = jax.ShapeDtypeStruct((24, 8, 128), BF16)
    hbm = pl.BlockSpec(memory_space=pltpu.HBM)
    own, one, two, three = pl.pallas_call(
        pack_kernel,
        out_shape=[window] * 4,
        in_specs=[hbm, hbm],
        scratch_shapes=[
            pltpu.VMEM((VARS, 8, 256), BF16),
            pltpu.VMEM((VARS, 8, 256), BF16),
            pltpu.VMEM((4, 192, 128), F32),
            pltpu.SemaphoreType.DMA((2,)),
        ],
        compiler_params=pltpu.CompilerParams(vmem_limit_bytes=4 << 20),
        name="pack",
    )(pinned(start), pinned(prior_mean))
    weights = pl.pallas_call(
        load_kernel,
        out_shape=[
            jax.ShapeDtypeStruct((256, 256), BF16),
            jax.ShapeDtypeStruct((1536, 256), BF16),
            jax.ShapeDtypeStruct((256, 256), BF16),
            jax.ShapeDtypeStruct((9, 256, 256), BF16),
            jax.ShapeDtypeStruct((9, 256, 256), BF16),
            jax.ShapeDtypeStruct((256, 256), BF16),
            jax.ShapeDtypeStruct((1536, 256), BF16),
            jax.ShapeDtypeStruct((256, 256), BF16),
        ],
        in_specs=[pl.BlockSpec(memory_space=pl.ANY)] + [hbm] * 8,
        scratch_shapes=[
            pltpu.VMEM((24, C0), BF16),
            pltpu.VMEM((C0, C1), BF16),
            pltpu.VMEM((C1, C0), BF16),
            pltpu.VMEM((VARS, C0), BF16),
            pltpu.SemaphoreType.DMA((42,)),
        ],
        compiler_params=pltpu.CompilerParams(vmem_limit_bytes=4 << 20),
        cost_estimate=pl.CostEstimate(flops=200000000, transcendentals=0, bytes_accessed=8000000),
        name="load",
    )(own, *map(pinned, (lift_w, conv0a, expand, conv1a, conv1b, shrink, conv0b, jnp.swapaxes(head, 1, 2))))
    one, two, three = (
        lax.ppermute(x, "lat", [(i, i ^ k) for i in range(lats)]) for k, x in ((1, one), (2, two), (3, three))
    )
    state, edge = pl.pallas_call(
        gather_kernel,
        out_shape=[
            jax.ShapeDtypeStruct((COLS * 16, 128), BF16),
            jax.ShapeDtypeStruct((KEPT * 16, 128), BF16),
        ],
        scratch_shapes=[pltpu.VMEM((4, 192, 128), F32), pltpu.VMEM((COLS * 16, 128), F32)],
        compiler_params=pltpu.CompilerParams(vmem_limit_bytes=8 << 20),
        name="gather",
    )(own, one, two, three)
    pairs = []
    for j in range(lons):
        lat = 3 if j % 2 == 0 else 0
        here, there = lat * lons + j, lat * lons + (j + 1) % lons
        pairs += [(here, there), (there, here)]
    edge = lax.ppermute(edge, ("lat", "lon"), pairs)
    piece = jax.ShapeDtypeStruct((VARS, 8, TILE), BF16)
    n1, n2 = TILE + 2 * HALO1, TILE + 2 * HALO2
    pieces = pl.pallas_call(
        network_kernel,
        out_shape=[piece] * 4,
        scratch_shapes=[
            pltpu.VMEM((COLS * 16, 128), F32),
            pltpu.VMEM((n1 * 16, 128), BF16),
            pltpu.VMEM((n1 * 16, 512), BF16),
            pltpu.VMEM(((n1 - 2) * 16, 256), BF16),
            pltpu.VMEM(((n1 - 2) * 8, 256), BF16),
            pltpu.VMEM(((n1 - 2) * 8, 768), BF16),
            pltpu.VMEM(((n1 - 6) * 8, 768), BF16),
            pltpu.VMEM(((n1 - 10) * 8, 256), BF16),
            pltpu.VMEM(((n1 - 10) * 16, 512), BF16),
            pltpu.VMEM((n2 * 16, 256), BF16),
            pltpu.VMEM((n2 * 16, 128), F32),
            pltpu.VMEM((TILE * 16, 128), F32),
            pltpu.VMEM((4, 96, TILE), F32),
        ],
        compiler_params=pltpu.CompilerParams(vmem_limit_bytes=24 << 20),
        name="networks",
    )(state, edge, noise_gain, *weights)
    pieces = [
        lax.ppermute(
            x, ("section", "lat"), [(s * lats + i, (1 - s) * lats + (i ^ k)) for s in range(2) for i in range(lats)]
        )
        for k, x in enumerate(pieces)
    ]
    return pl.pallas_call(
        place_kernel,
        out_shape=jax.ShapeDtypeStruct((1,) + prior_mean.shape, BF16),
        compiler_params=pltpu.CompilerParams(vmem_limit_bytes=4 << 20),
        name="place",
    )(*pieces)


def solution(mesh):
    placed = (
        P("section", None, "lat", "lon"),
        P(None, "lat", "lon"),
        P("section", None, None),
        P("section", None),
        P("section", None, None, None),
        P("section", None, None),
        P("section", None, None, None),
        P("section", None, None, None),
        P("section", None, None),
        P("section", None, None, None),
        P("section", None, None),
    )
    return jax.shard_map(
        on_device,
        mesh=mesh,
        in_specs=placed,
        out_specs=P("section", None, "lat", "lon"),
        check_vma=False,
    )
```
